32 devices in a mesh: text: 16 (over z, y, x), query: 2 (over core).
Axes of the slice: x: 2, y: 2, z: 4, core: 2. Of those that a mesh axis runs over, the one named last changes fastest.
Arguments:
- query_embed: bfloat16 [1024, 1024], P(('text', 'query')), may hold values from -6 to 6
- truth_ids: int32 [1024], P(('text', 'query')), may hold values from 0 to 8191
- text_embed: bfloat16 [8192, 1024], P('text'), may hold values from -0.1875 to 0.1875
- text_ids: int32 [8192], P('text'), may hold values from 0 to 8191, each once
Outputs:
- top_scores: float32 [1024, 10], P(('text', 'query'))
- margins: float32 [1024, 3], P(('text', 'query'))
The draws below stay inside these ranges and needn't reach their ends.
Inputs may be any that keep to these rules, and one draw needn't show every extreme that they name: `text_ids`: every id of 0 to 8191 stands in exactly one row.
All inputs are finite; a program needn't handle non-finite values.
Results may differ from the reference program's by a relative error of at most 0.0003.
Values may be sent and summed in bfloat16 or wider, within the bound.
No kernel may reach another device: no remote copies, remote signals or barrier semaphores. Data moves between devices by JAX's collectives and lax.ppermute only.
A program may use at most 64 MiB of HBM per device.

```python
import jax
import jax.numpy as jnp
from jax import lax

D = 1024
TOPK = 10
NQ = 1024
NT = 8192


def set_ends(entries, stream_key, least, largest):
    longest = entries.shape.index(max(entries.shape))
    spots = []
    for shift in (0, 1):
        where = [jax.random.randint(jax.random.fold_in(stream_key, axis), (), 0, length) for axis, length in enumerate(entries.shape)]
        where[longest] = (where[longest] + shift) % entries.shape[longest]
        spots.append(tuple(where))
    return entries.at[spots[0]].set(least).at[spots[1]].set(largest)


def level_of(key, extent, pieces, least, largest):
    gain, own = 1.0, jax.random.fold_in(key, 6)
    for position, parts in pieces:
        draws = jnp.exp(jax.random.uniform(jax.random.fold_in(own, position), (parts,), jnp.float32, least / len(pieces), largest / len(pieces)))
        gain = gain * jnp.repeat(draws, extent[position] // parts).reshape([-1 if axis == position else 1 for axis in range(len(extent))])
    return gain


def centred(key, dims, width, limit, pieces=(), held_as=jnp.bfloat16):
    drawn = jax.random.normal(key, dims, jnp.float32) * width
    if len(pieces) > 0:
        drawn = level_of(key, dims, pieces, -0.22, 0.18) * drawn
    return jnp.clip(drawn, min=-limit, max=limit).astype(held_as)


def setup_inputs(seed: int = 0) -> dict:
    seeds = jax.random.split(jax.random.key(seed), 5)
    query_embed = centred(seeds[0], (NQ, D), 1.0, 6.0, ((0, 32),))
    truth_ids = set_ends(jax.random.randint(seeds[1], (NQ,), 0, NT), jax.random.fold_in(seeds[1], 1), 0, NT - 1).astype(jnp.int32)
    text_embed = centred(seeds[2], (NT, D), D ** -0.5, 0.1875, ((0, 16),))
    text_ids = jax.random.permutation(seeds[3], NT).astype(jnp.int32)
    return dict(query_embed=query_embed, truth_ids=truth_ids, text_embed=text_embed, text_ids=text_ids)


def rank_block(query_slab, text_embed):
    scores = lax.dot_general(query_slab, text_embed, (((1,), (1,)), ((), ())), preferred_element_type=jnp.float32)
    return lax.top_k(scores, TOPK)[0]


def reference(query_embed, truth_ids, text_embed, text_ids):
    inverse = jnp.zeros((NT,), jnp.int32).at[text_ids].set(jnp.arange(NT, dtype=jnp.int32))
    matched = text_embed[inverse[truth_ids]]
    truth_score = jnp.sum(query_embed.astype(jnp.float32) * matched.astype(jnp.float32), axis=1)
    block_rows = min(512, NQ)
    blocks = query_embed.reshape(NQ // block_rows, block_rows, D)
    ranked = lax.map(lambda query_slab: rank_block(query_slab, text_embed), blocks)
    top_scores = ranked.reshape(NQ, TOPK)
    margins = jnp.stack([truth_score - top_scores[:, 0], truth_score - top_scores[:, 4], truth_score - top_scores[:, 9]], axis=1)
    return top_scores, margins
```

```python
import jax
import jax.numpy as jnp
from jax import lax
from jax.experimental import pallas as pl
from jax.experimental.pallas import tpu as pltpu
from jax.sharding import PartitionSpec as P

TOPK = 10
LANES = 128
PLANE = 4
PAIR = 4


def exchange(c, i, j):
    c[i], c[j] = jnp.maximum(c[i], c[j]), jnp.minimum(c[i], c[j])


def sort_pairs(n):
    pairs = []
    p = 1
    while p < n:
        k = p
        while k >= 1:
            for j in range(k % p, n - k, 2 * k):
                for i in range(min(k, n - j - k)):
                    if (i + j) // (2 * p) == (i + j + k) // (2 * p):
                        pairs.append((i + j, i + j + k))
            k //= 2
        p *= 2
    return pairs


def sort_top(values):
    c = list(values)
    for i, j in sort_pairs(len(c)):
        exchange(c, i, j)
    return c[:TOPK]


def merge_top(a, b):
    c = [jnp.maximum(a[i], b[TOPK - 1 - i]) for i in range(TOPK)]
    exchange(c, 0, 8)
    exchange(c, 1, 9)
    head = [jnp.maximum(c[0], c[1]), jnp.minimum(c[0], c[1])]
    tail = [c[8], c[9]] + c[2:8]
    for step in (4, 2, 1):
        for i in range(8):
            if i & step == 0:
                exchange(tail, i, i + step)
    return head + tail


def pack_queries(query_ref, ids_ref, out_ref):
    rows, depth = query_ref.shape
    columns = depth // LANES
    for j in range(columns):
        out_ref[0, j * rows : (j + 1) * rows, :] = query_ref[:, j * LANES : (j + 1) * LANES]
    ids = jnp.concatenate([ids_ref[...], jnp.zeros((1, LANES - rows), jnp.int32)], axis=1)
    high = (ids >> 8).astype(jnp.float32)
    low = (ids & 255).astype(jnp.float32)
    row = lax.broadcasted_iota(jnp.int32, (16, LANES), 0)
    digits = jnp.where(row == 0, high, jnp.where(row == 1, low, 0.0))
    out_ref[0, columns * rows :, :] = digits.astype(jnp.bfloat16)


def pack_texts(core_ref, text_ref, ids_ref, out_ref):
    half, depth = text_ref.shape
    out_ref[:half, :] = text_ref[...]
    row = lax.broadcasted_iota(jnp.int32, (16, half), 0)
    ids = ids_ref[...]
    high = (ids >> 8).astype(jnp.float32)
    low = (ids & 255).astype(jnp.float32)
    digits = jnp.where(row == 0, high, jnp.where(row == 1, low, 0.0))
    out_ref[half:, :half] = digits.astype(jnp.bfloat16)
    out_ref[half:, half:] = jnp.zeros((16, depth - half), jnp.bfloat16)


def rank(*refs, tiles, rows):
    text_ref, ids_ref, near_ref, far_ref = refs[:4]
    bundles = refs[4 : 4 + PLANE]
    outs = refs[4 + PLANE : 4 + PLANE + tiles]
    query_ref, score_ref, label_ref = refs[4 + PLANE + tiles :]
    depth = text_ref.shape[1]
    columns = depth // LANES
    width = PLANE * rows
    own = text_ref.shape[0]
    half = near_ref.shape[0] - 16

    def spread(row, start):
        for i in range(0, row.shape[1], LANES):
            block = jnp.broadcast_to(row[:, i : i + LANES], (LANES, LANES))
            label_ref[start + i : start + i + LANES, :] = block.T

    spread(ids_ref[...].astype(jnp.float32), 0)
    for n, ref in enumerate((near_ref, far_ref)):
        digits = ref[half:, :half].astype(jnp.float32)
        spread(digits[0:1] * 256.0 + digits[1:2], own + n * half)

    wanted = []
    for h in range(tiles):
        total = jnp.zeros((1, LANES), jnp.float32)
        for d in range(PLANE):
            for j in range(columns):
                query_ref[
                    h * width + d * rows : h * width + (d + 1) * rows, j * LANES : (j + 1) * LANES
                ] = bundles[d][h, j * rows : (j + 1) * rows, :]
            digits = bundles[d][h, columns * rows :, :].astype(jnp.float32)
            here = digits[0:1] * 256.0 + digits[1:2]
            total = total + (here if d == 0 else pltpu.roll(here, d * rows, 1))
        wanted.append(jnp.broadcast_to(total, (8, LANES)))

    queries = query_ref[...]
    pieces = [(text_ref, own, 0), (near_ref, half, own), (far_ref, half, own + half)]
    for ref, count, start in pieces:
        for r in range(0, count, half):
            score_ref[start + r : start + r + half, :] = lax.dot_general(
                ref[r : r + half, :],
                queries,
                (((1,), (1,)), ((), ())),
                preferred_element_type=jnp.float32,
            )
    groups = (own + 2 * half) // LANES
    for h in range(tiles):
        lanes = slice(h * width, (h + 1) * width)

        def step(g, carry):
            best, truth = list(carry[:TOPK]), carry[TOPK]
            values = []
            for i in range(16):
                at = pl.ds(pl.multiple_of(g * LANES + i * 8, 8), 8)
                s = score_ref[at, lanes]
                truth = truth + jnp.where(label_ref[at, :] == wanted[h], s, 0.0)
                values.append(s)
            return tuple(merge_top(best, sort_top(values))) + (truth,)

        low = jnp.full((8, width), -jnp.inf, jnp.float32)
        carry = (low,) * TOPK + (jnp.zeros((8, width), jnp.float32),)
        carry = lax.fori_loop(0, groups, step, carry)
        best, truth = list(carry[:TOPK]), carry[TOPK]
        for shift in (4, 2, 1):
            best = merge_top(best, [pltpu.roll(b, shift, 0) for b in best])
        for i in range(TOPK):
            outs[h][i : i + 1, :] = best[i][0:1, :]
        outs[h][TOPK : TOPK + 1, :] = jnp.sum(truth, axis=0, keepdims=True)
        outs[h][TOPK + 1 :, :] = jnp.zeros((16 - TOPK - 1, width), jnp.float32)


def join(ours_ref, theirs_ref, out_ref):
    best = merge_top(
        [ours_ref[i : i + 1, :] for i in range(TOPK)], [theirs_ref[i : i + 1, :] for i in range(TOPK)]
    )
    for i in range(TOPK):
        out_ref[i : i + 1, :] = best[i]
    out_ref[TOPK : TOPK + 1, :] = ours_ref[TOPK : TOPK + 1, :] + theirs_ref[TOPK : TOPK + 1, :]
    out_ref[TOPK + 1 :, :] = jnp.zeros_like(out_ref[TOPK + 1 :, :])


def finish(*refs, rows):
    lists = []
    for d in range(PLANE):
        x = refs[d][...]
        lists.append(x if d == 0 else pltpu.roll(x, LANES - d * rows, 1))
    top_ref, margin_ref = refs[PLANE:]
    ranks = [[x[i : i + 1, :] for i in range(TOPK)] for x in lists]
    best = merge_top(merge_top(ranks[0], ranks[1]), merge_top(ranks[2], ranks[3]))
    truth = lists[0] + lists[1] + lists[2] + lists[3]
    truth = truth[TOPK : TOPK + 1, :]
    for i in range(TOPK):
        top_ref[i : i + 1, :] = best[i][:, :rows]
    for i, k in enumerate((0, 4, 9)):
        margin_ref[i : i + 1, :] = (truth - best[k])[:, :rows]


def per_device(query_embed, truth_ids, text_embed, text_ids, texts, cores):
    rows, depth = query_embed.shape
    own = text_embed.shape[0]
    half = own // 2
    f32 = jnp.float32

    def permute(x, s):
        return lax.ppermute(x, "text", [(i, i ^ s) for i in range(texts)])

    side = lax.rem(lax.axis_index("query"), 2)
    sent = pl.pallas_call(
        pack_texts,
        grid_spec=pltpu.PrefetchScalarGridSpec(
            num_scalar_prefetch=1,
            grid=(1,),
            in_specs=[
                pl.BlockSpec((half, depth), lambda i, c: (c[0], 0)),
                pl.BlockSpec((1, half), lambda i, c: (0, c[0])),
            ],
            out_specs=pl.BlockSpec((half + 16, depth), lambda i, c: (0, 0)),
        ),
        out_shape=jax.ShapeDtypeStruct((half + 16, depth), jnp.bfloat16),
        name="pack_texts",
    )(side.reshape(1), text_embed, text_ids.reshape(1, own))
    near = permute(sent, PAIR)
    far = lax.ppermute(near, "query", [(i, i ^ 1) for i in range(cores)])

    packed = (depth // LANES) * rows + 16
    bundle = pl.pallas_call(
        pack_queries,
        out_shape=jax.ShapeDtypeStruct((1, packed, LANES), jnp.bfloat16),
        name="pack_queries",
    )(query_embed, truth_ids.reshape(1, rows))
    far_bits = []
    s = PAIR * 2
    while s < texts:
        far_bits.append(s)
        s *= 2
    for s in far_bits:
        bundle = jnp.concatenate([bundle, permute(bundle, s)], axis=0)
    tiles = bundle.shape[0]
    bundles = [bundle] + [permute(bundle, d) for d in range(1, PLANE)]

    width = PLANE * rows
    lists = pl.pallas_call(
        lambda *refs: rank(*refs, tiles=tiles, rows=rows),
        out_shape=[jax.ShapeDtypeStruct((16, width), f32)] * tiles,
        scratch_shapes=[
            pltpu.VMEM((tiles * width, depth), jnp.bfloat16),
            pltpu.VMEM((2 * own, tiles * width), f32),
            pltpu.VMEM((2 * own, LANES), f32),
        ],
        name="rank",
    )(text_embed, text_ids.reshape(1, own), near, far, *bundles)
    lists = list(lists)
    for s in reversed(far_bits):
        mid = len(lists) // 2
        lists = [
            pl.pallas_call(join, out_shape=jax.ShapeDtypeStruct((16, width), f32), name="join")(
                lists[t], permute(lists[mid + t], s)
            )
            for t in range(mid)
        ]
    mine = lists[0]
    top, margins = pl.pallas_call(
        lambda *refs: finish(*refs, rows=rows),
        out_shape=[jax.ShapeDtypeStruct((TOPK, rows), f32), jax.ShapeDtypeStruct((3, rows), f32)],
        name="finish",
    )(mine, *[permute(mine, d) for d in range(1, PLANE)])
    return top.T, margins.T


def solution(mesh):
    texts, cores = mesh.shape["text"], mesh.shape["query"]
    return jax.shard_map(
        lambda *args: per_device(*args, texts=texts, cores=cores),
        mesh=mesh,
        in_specs=(P(("text", "query"), None), P(("text", "query")), P("text", None), P("text")),
        out_specs=(P(("text", "query"), None), P(("text", "query"), None)),
        check_vma=False,
    )
```

```python
import jax
import jax.numpy as jnp
from jax import lax
from jax.experimental import pallas as pl
from jax.experimental.pallas import tpu as pltpu
from jax.sharding import PartitionSpec as P

TOPK = 10
LANES = 128
PLANE = 4
PAIR = 4


def exchange(c, i, j):
    c[i], c[j] = jnp.maximum(c[i], c[j]), jnp.minimum(c[i], c[j])


def sort_pairs(n):
    pairs = []
    p = 1
    while p < n:
        k = p
        while k >= 1:
            for j in range(k % p, n - k, 2 * k):
                for i in range(min(k, n - j - k)):
                    if (i + j) // (2 * p) == (i + j + k) // (2 * p):
                        pairs.append((i + j, i + j + k))
            k //= 2
        p *= 2
    return pairs


def sort_top(values):
    c = list(values)
    for i, j in sort_pairs(len(c)):
        exchange(c, i, j)
    return c[:TOPK]


def merge_top(a, b):
    c = [jnp.maximum(a[i], b[TOPK - 1 - i]) for i in range(TOPK)]
    exchange(c, 0, 8)
    exchange(c, 1, 9)
    head = [jnp.maximum(c[0], c[1]), jnp.minimum(c[0], c[1])]
    tail = [c[8], c[9]] + c[2:8]
    for step in (4, 2, 1):
        for i in range(8):
            if i & step == 0:
                exchange(tail, i, i + step)
    return head + tail


def pack_queries(query_ref, ids_ref, out_ref):
    rows, depth = query_ref.shape
    columns = depth // LANES
    for j in range(columns):
        out_ref[0, j * rows : (j + 1) * rows, :] = query_ref[:, j * LANES : (j + 1) * LANES]
    ids = jnp.concatenate([ids_ref[...], jnp.zeros((1, LANES - rows), jnp.int32)], axis=1)
    high = (ids >> 8).astype(jnp.float32)
    low = (ids & 255).astype(jnp.float32)
    row = lax.broadcasted_iota(jnp.int32, (16, LANES), 0)
    digits = jnp.where(row == 0, high, jnp.where(row == 1, low, 0.0))
    out_ref[0, columns * rows :, :] = digits.astype(jnp.bfloat16)


def pack_texts(core_ref, text_ref, ids_ref, out_ref):
    half, depth = text_ref.shape
    out_ref[:half, :] = text_ref[...]
    row = lax.broadcasted_iota(jnp.int32, (16, half), 0)
    ids = ids_ref[...]
    high = (ids >> 8).astype(jnp.float32)
    low = (ids & 255).astype(jnp.float32)
    digits = jnp.where(row == 0, high, jnp.where(row == 1, low, 0.0))
    out_ref[half:, :half] = digits.astype(jnp.bfloat16)
    out_ref[half:, half:] = jnp.zeros((16, depth - half), jnp.bfloat16)


def scan(text_ref, queries, label_ref, score_ref, wanted, states):
    count = score_ref.shape[0]
    piece = min(count, 2 * LANES)
    for r in range(0, count, piece):
        score_ref[r : r + piece, :] = lax.dot_general(
            text_ref[r : r + piece, :],
            queries,
            (((1,), (1,)), ((), ())),
            preferred_element_type=jnp.float32,
        )
    results = []
    for h, state in enumerate(states):
        lanes = slice(h * LANES, (h + 1) * LANES)

        def step(g, carry):
            best, truth = list(carry[:TOPK]), carry[TOPK]
            values = []
            for i in range(16):
                at = pl.ds(pl.multiple_of(g * LANES + i * 8, 8), 8)
                s = score_ref[at, lanes]
                truth = truth + jnp.where(label_ref[at, :] == wanted[h], s, 0.0)
                values.append(s)
            return tuple(merge_top(best, sort_top(values))) + (truth,)

        results.append(lax.fori_loop(0, count // LANES, step, tuple(state)))
    return results


def spread(row, label_ref):
    for i in range(0, row.shape[1], LANES):
        label_ref[i : i + LANES, :] = jnp.broadcast_to(row[:, i : i + LANES], (LANES, LANES)).T


def joined(digits):
    digits = digits.astype(jnp.float32)
    return digits[0:1] * 256.0 + digits[1:2]


def rank_own(*refs, tiles, rows):
    text_ref, ids_ref = refs[:2]
    bundles = refs[2 : 2 + PLANE]
    query_ref, wanted_ref, state_ref, score_ref, label_ref = refs[2 + PLANE :]
    columns = text_ref.shape[1] // LANES
    spread(ids_ref[...].astype(jnp.float32), label_ref)
    wanted = []
    for h in range(tiles):
        total = jnp.zeros((1, LANES), jnp.float32)
        for d in range(PLANE):
            at = slice(h * LANES + d * rows, h * LANES + (d + 1) * rows)
            for j in range(columns):
                block = bundles[d][h, j * rows : (j + 1) * rows, :]
                query_ref[at, j * LANES : (j + 1) * LANES] = block
            here = joined(bundles[d][h, columns * rows :, :])
            total = total + (here if d == 0 else pltpu.roll(here, d * rows, 1))
        wanted.append(jnp.broadcast_to(total, (8, LANES)))
        wanted_ref[h] = wanted[h]
    low = jnp.full((8, LANES), -jnp.inf, jnp.float32)
    start = [low] * TOPK + [jnp.zeros((8, LANES), jnp.float32)]
    states = scan(text_ref, query_ref[...], label_ref, score_ref, wanted, [start] * tiles)
    for h in range(tiles):
        for i in range(TOPK + 1):
            state_ref[h, i] = states[h][i]


def scan_more(part_ref, query_ref, wanted_ref, state_ref, score_ref, label_ref):
    half = part_ref.shape[0] - 16
    tiles = state_ref.shape[0]
    spread(joined(part_ref[half:, :half]), label_ref)
    wanted = [wanted_ref[h] for h in range(tiles)]
    states = [[state_ref[h, i] for i in range(TOPK + 1)] for h in range(tiles)]
    return scan(part_ref, query_ref[...], label_ref, score_ref, wanted, states)


def rank_near(near_ref, query_ref, wanted_ref, state_ref, next_ref, score_ref, label_ref):
    states = scan_more(near_ref, query_ref, wanted_ref, state_ref, score_ref, label_ref)
    for h, state in enumerate(states):
        for i in range(TOPK + 1):
            next_ref[h, i] = state[i]


def rank_far(far_ref, query_ref, wanted_ref, state_ref, *refs):
    outs, (score_ref, label_ref) = refs[:-2], refs[-2:]
    states = scan_more(far_ref, query_ref, wanted_ref, state_ref, score_ref, label_ref)
    for out_ref, state in zip(outs, states):
        best, truth = list(state[:TOPK]), state[TOPK]
        for shift in (4, 2, 1):
            best = merge_top(best, [pltpu.roll(b, shift, 0) for b in best])
        for i in range(TOPK):
            out_ref[i : i + 1, :] = best[i][0:1, :]
        out_ref[TOPK : TOPK + 1, :] = jnp.sum(truth, axis=0, keepdims=True)
        out_ref[TOPK + 1 :, :] = jnp.zeros((16 - TOPK - 1, LANES), jnp.float32)


def join(ours_ref, theirs_ref, out_ref):
    best = merge_top(
        [ours_ref[i : i + 1, :] for i in range(TOPK)], [theirs_ref[i : i + 1, :] for i in range(TOPK)]
    )
    for i in range(TOPK):
        out_ref[i : i + 1, :] = best[i]
    out_ref[TOPK : TOPK + 1, :] = ours_ref[TOPK : TOPK + 1, :] + theirs_ref[TOPK : TOPK + 1, :]
    out_ref[TOPK + 1 :, :] = jnp.zeros_like(out_ref[TOPK + 1 :, :])


def finish(*refs, rows):
    lists = []
    for d in range(PLANE):
        x = refs[d][...]
        lists.append(x if d == 0 else pltpu.roll(x, LANES - d * rows, 1))
    top_ref, margin_ref = refs[PLANE:]
    ranks = [[x[i : i + 1, :] for i in range(TOPK)] for x in lists]
    best = merge_top(merge_top(ranks[0], ranks[1]), merge_top(ranks[2], ranks[3]))
    truth = lists[0] + lists[1] + lists[2] + lists[3]
    truth = truth[TOPK : TOPK + 1, :]
    for i in range(TOPK):
        top_ref[i : i + 1, :] = best[i][:, :rows]
    for i, k in enumerate((0, 4, 9)):
        margin_ref[i : i + 1, :] = (truth - best[k])[:, :rows]


def kernel(body, out_shape, mib, flops=0, **extra):
    size = sum(x.size * x.dtype.itemsize for x in jax.tree.leaves(out_shape))
    return pl.pallas_call(
        body,
        out_shape=out_shape,
        compiler_params=pltpu.CompilerParams(vmem_limit_bytes=mib << 20),
        cost_estimate=pl.CostEstimate(flops=flops, bytes_accessed=size, transcendentals=0),
        **extra,
    )


def per_device(query_embed, truth_ids, text_embed, text_ids, texts, cores):
    rows, depth = query_embed.shape
    own = text_embed.shape[0]
    half = own // 2
    f32, bf16 = jnp.float32, jnp.bfloat16

    def permute(x, s):
        return lax.ppermute(x, "text", [(i, i ^ s) for i in range(texts)])

    packed = (depth // LANES) * rows + 16
    bundle = kernel(
        pack_queries, jax.ShapeDtypeStruct((1, packed, LANES), bf16), 4
    )(query_embed, truth_ids.reshape(1, rows))
    side = lax.rem(lax.axis_index("query"), 2)
    sent = kernel(
        pack_texts,
        jax.ShapeDtypeStruct((half + 16, depth), bf16),
        4,
        grid_spec=pltpu.PrefetchScalarGridSpec(
            num_scalar_prefetch=1,
            grid=(1,),
            in_specs=[
                pl.BlockSpec((half, depth), lambda i, c: (c[0], 0)),
                pl.BlockSpec((1, half), lambda i, c: (0, c[0])),
            ],
            out_specs=pl.BlockSpec((half + 16, depth), lambda i, c: (0, 0)),
        ),
    )(side.reshape(1), text_embed, text_ids.reshape(1, own))

    far_bits = []
    s = PAIR * 2
    while s < texts:
        far_bits.append(s)
        s *= 2
    for s in far_bits:
        bundle = jnp.concatenate([bundle, permute(bundle, s)], axis=0)
    near = permute(sent, PAIR)
    tiles = bundle.shape[0]
    bundles = [bundle] + [permute(bundle, d) for d in range(1, PLANE)]

    state_shape = jax.ShapeDtypeStruct((tiles, TOPK + 1, 8, LANES), f32)
    list_shape = jax.ShapeDtypeStruct((16, LANES), f32)
    flops = 2 * own * tiles * LANES * depth
    queries, wanted, state = kernel(
        lambda *refs: rank_own(*refs, tiles=tiles, rows=rows),
        [
            jax.ShapeDtypeStruct((tiles * LANES, depth), bf16),
            jax.ShapeDtypeStruct((tiles, 8, LANES), f32),
            state_shape,
        ],
        12,
        flops=flops,
        scratch_shapes=[pltpu.VMEM((own, tiles * LANES), f32), pltpu.VMEM((own, LANES), f32)],
    )(text_embed, text_ids.reshape(1, own), *bundles)
    far = lax.ppermute(near, "query", [(i, i ^ 1) for i in range(cores)])
    scratch = [pltpu.VMEM((half, tiles * LANES), f32), pltpu.VMEM((half, LANES), f32)]
    state = kernel(
        rank_near, state_shape, 8, flops=flops // 2, scratch_shapes=scratch
    )(near, queries, wanted, state)
    lists = kernel(
        rank_far, [list_shape] * tiles, 8, flops=flops // 2, scratch_shapes=scratch
    )(far, queries, wanted, state)
    lists = list(lists)
    for s in reversed(far_bits):
        mid = len(lists) // 2
        lists = [
            kernel(join, list_shape, 1)(lists[t], permute(lists[mid + t], s))
            for t in range(mid)
        ]
    mine = lists[0]
    top, margins = kernel(
        lambda *refs: finish(*refs, rows=rows),
        [jax.ShapeDtypeStruct((TOPK, rows), f32), jax.ShapeDtypeStruct((3, rows), f32)],
        1,
    )(mine, *[permute(mine, d) for d in range(1, PLANE)])
    return top.T, margins.T


def solution(mesh):
    texts, cores = mesh.shape["text"], mesh.shape["query"]
    return jax.shard_map(
        lambda *args: per_device(*args, texts=texts, cores=cores),
        mesh=mesh,
        in_specs=(P(("text", "query"), None), P(("text", "query")), P("text", None), P("text")),
        out_specs=(P(("text", "query"), None), P(("text", "query"), None)),
        check_vma=False,
    )
```

```python
import jax
import jax.numpy as jnp
from jax import lax
from jax.experimental import pallas as pl
from jax.experimental.pallas import tpu as pltpu
from jax.sharding import PartitionSpec as P

TOPK = 10
LANES = 128
PLANE = 4
PARTS = 2
PAIR = 4


def exchange(c, i, j):
    c[i], c[j] = jnp.maximum(c[i], c[j]), jnp.minimum(c[i], c[j])


def sort_pairs(n):
    pairs = []
    p = 1
    while p < n:
        k = p
        while k >= 1:
            for j in range(k % p, n - k, 2 * k):
                for i in range(min(k, n - j - k)):
                    if (i + j) // (2 * p) == (i + j + k) // (2 * p):
                        pairs.append((i + j, i + j + k))
            k //= 2
        p *= 2
    return pairs


def sort_top(values):
    c = list(values)
    for i, j in sort_pairs(len(c)):
        exchange(c, i, j)
    return c[:TOPK]


def merge_top(a, b):
    c = [jnp.maximum(a[i], b[TOPK - 1 - i]) for i in range(TOPK)]
    exchange(c, 0, 8)
    exchange(c, 1, 9)
    head = [jnp.maximum(c[0], c[1]), jnp.minimum(c[0], c[1])]
    tail = [c[8], c[9]] + c[2:8]
    for step in (4, 2, 1):
        for i in range(8):
            if i & step == 0:
                exchange(tail, i, i + step)
    return head + tail


def digits_of(ids):
    high = (ids >> 8).astype(jnp.float32)
    low = (ids & 255).astype(jnp.float32)
    row = lax.broadcasted_iota(jnp.int32, (16, ids.shape[1]), 0)
    return jnp.where(row == 0, high, jnp.where(row == 1, low, 0.0)).astype(jnp.bfloat16)


def pack_queries(query_ref, wanted_ref, block_ref):
    rows, depth = query_ref.shape
    columns = depth // LANES
    for j in range(columns):
        block_ref[0, j * rows : (j + 1) * rows, :] = query_ref[:, j * LANES : (j + 1) * LANES]
    ids = jnp.concatenate([wanted_ref[...], jnp.zeros((1, LANES - rows), jnp.int32)], axis=1)
    block_ref[0, columns * rows :, :] = digits_of(ids)


def pack_texts(text_ref, ids_ref, *part_refs):
    part, depth = part_refs[-1].shape[0] - (8 if len(part_refs) == 1 else 0), text_ref.shape[1]
    half = part * len(part_refs)
    start = pl.multiple_of(lax.rem(lax.axis_index("query"), 2) * half, half)
    for n, part_ref in enumerate(part_refs):
        part_ref[:part, :] = text_ref[pl.ds(pl.multiple_of(start + n * part, part), part), :]
    first_ref = part_refs[0]
    first_ref[part:, :half] = digits_of(ids_ref[:, pl.ds(start, half)])[:8]
    first_ref[part:, half:] = jnp.zeros((8, depth - half), jnp.bfloat16)


def scan(text_ref, queries, label_ref, score_ref, wanted, states):
    count = score_ref.shape[0]
    piece = min(count, 2 * LANES)
    for r in range(0, count, piece):
        score_ref[r : r + piece, :] = lax.dot_general(
            text_ref[r : r + piece, :],
            queries,
            (((1,), (1,)), ((), ())),
            preferred_element_type=jnp.float32,
        )
    results = []
    for h, state in enumerate(states):
        lanes = slice(h * LANES, (h + 1) * LANES)

        def step(g, carry):
            best, truth = list(carry[:TOPK]), carry[TOPK]
            values = []
            for i in range(16):
                at = pl.ds(pl.multiple_of(g * LANES + i * 8, 8), 8)
                s = score_ref[at, lanes]
                truth = truth + jnp.where(label_ref[at, :] == wanted[h], s, 0.0)
                values.append(s)
            return tuple(merge_top(best, sort_top(values))) + (truth,)

        results.append(lax.fori_loop(0, count // LANES, step, tuple(state)))
    return results


def spread(row, label_ref):
    for i in range(0, row.shape[1], LANES):
        label_ref[i : i + LANES, :] = jnp.broadcast_to(row[:, i : i + LANES], (LANES, LANES)).T


def joined(digits):
    digits = digits.astype(jnp.float32)
    return digits[0:1] * 256.0 + digits[1:2]


def blank(state_ref):
    for i in range(TOPK + 1):
        state_ref[i] = jnp.full((8, LANES), -jnp.inf if i < TOPK else 0.0, jnp.float32)


def rank_own(*refs, tiles, rows):
    text_ref, ids_ref, blank_ref = refs[:3]
    refs = refs[1:]
    bundles = refs[2 : 2 + PLANE]
    query_ref, wanted_ref, state_ref, score_ref, label_ref = refs[2 + PLANE :]
    columns = text_ref.shape[1] // LANES
    spread(ids_ref[...].astype(jnp.float32), label_ref)
    wanted = []
    for h in range(tiles):
        total = jnp.zeros((1, LANES), jnp.float32)
        for d in range(PLANE):
            at = slice(h * LANES + d * rows, h * LANES + (d + 1) * rows)
            source = bundles[d].at[h]
            for j in range(columns):
                query_ref[at, j * LANES : (j + 1) * LANES] = source[j * rows : (j + 1) * rows, :]
            here = joined(source[columns * rows :, :])
            total = total + (here if d == 0 else pltpu.roll(here, d * rows, 1))
        wanted.append(jnp.broadcast_to(total, (8, LANES)))
        wanted_ref[h] = wanted[h]
    start = [blank_ref[i] for i in range(TOPK + 1)]
    states = scan(text_ref, query_ref[...], label_ref, score_ref, wanted, [start] * tiles)
    for h in range(tiles):
        for i in range(TOPK + 1):
            state_ref[h, i] = states[h][i]


def load_states(wanted_ref, state_ref):
    tiles = state_ref.shape[0]
    wanted = [wanted_ref[h] for h in range(tiles)]
    return wanted, [[state_ref[h, i] for i in range(TOPK + 1)] for h in range(tiles)]


def scan_part(part_ref, first_ref, count, query_ref, wanted, states, score_ref, label_ref, part):
    at = slice(part * count, (part + 1) * count)
    spread(joined(first_ref[count:, at]), label_ref)
    return scan(part_ref, query_ref[...], label_ref, score_ref, wanted, states)


def rank_parts(*refs, parts):
    part_refs, refs = refs[: len(parts)], refs[len(parts) :]
    first_refs, refs = refs[: len(parts)], refs[len(parts) :]
    query_ref, wanted_ref, state_ref, next_ref, score_ref, label_ref = refs
    count = score_ref.shape[0]
    wanted, states = load_states(wanted_ref, state_ref)
    for part_ref, first_ref, part in zip(part_refs, first_refs, parts):
        states = scan_part(
            part_ref, first_ref, count, query_ref, wanted, states, score_ref, label_ref, part
        )
    for h, state in enumerate(states):
        for i in range(TOPK + 1):
            next_ref[h, i] = state[i]


def rank_last(part_ref, first_ref, query_ref, wanted_ref, state_ref, *refs, part):
    outs, (score_ref, label_ref) = refs[:-2], refs[-2:]
    count = score_ref.shape[0]
    wanted, states = load_states(wanted_ref, state_ref)
    states = scan_part(
        part_ref, first_ref, count, query_ref, wanted, states, score_ref, label_ref, part
    )
    for out_ref, state in zip(outs, states):
        best, truth = list(state[:TOPK]), state[TOPK]
        for shift in (4, 2, 1):
            best = merge_top(best, [pltpu.roll(b, shift, 0) for b in best])
        for i in range(TOPK):
            out_ref[i : i + 1, :] = best[i][0:1, :]
        out_ref[TOPK : TOPK + 1, :] = jnp.sum(truth, axis=0, keepdims=True)
        out_ref[TOPK + 1 :, :] = jnp.zeros((16 - TOPK - 1, LANES), jnp.float32)


def join(ours_ref, theirs_ref, out_ref):
    best = merge_top(
        [ours_ref[i : i + 1, :] for i in range(TOPK)], [theirs_ref[i : i + 1, :] for i in range(TOPK)]
    )
    for i in range(TOPK):
        out_ref[i : i + 1, :] = best[i]
    out_ref[TOPK : TOPK + 1, :] = ours_ref[TOPK : TOPK + 1, :] + theirs_ref[TOPK : TOPK + 1, :]
    out_ref[TOPK + 1 :, :] = jnp.zeros_like(out_ref[TOPK + 1 :, :])


def finish(*refs, rows):
    lists = []
    for d in range(PLANE):
        x = refs[d][...]
        lists.append(x if d == 0 else pltpu.roll(x, LANES - d * rows, 1))
    top_ref, margin_ref = refs[PLANE:]
    ranks = [[x[i : i + 1, :] for i in range(TOPK)] for x in lists]
    best = merge_top(merge_top(ranks[0], ranks[1]), merge_top(ranks[2], ranks[3]))
    truth = lists[0] + lists[1] + lists[2] + lists[3]
    truth = truth[TOPK : TOPK + 1, :]
    for i in range(TOPK):
        top_ref[i : i + 1, :] = best[i][:, :rows]
    for i, k in enumerate((0, 4, 9)):
        margin_ref[i : i + 1, :] = (truth - best[k])[:, :rows]


def kernel(body, out_shape, mib, flops=0, **extra):
    size = sum(x.size * x.dtype.itemsize for x in jax.tree.leaves(out_shape))
    return pl.pallas_call(
        body,
        out_shape=out_shape,
        compiler_params=pltpu.CompilerParams(vmem_limit_bytes=mib << 20),
        cost_estimate=pl.CostEstimate(flops=flops, bytes_accessed=size, transcendentals=0),
        **extra,
    )


def per_device(query_embed, truth_ids, text_embed, text_ids, texts, cores):
    rows, depth = query_embed.shape
    own = text_embed.shape[0]
    f32, bf16 = jnp.float32, jnp.bfloat16

    def permute(x, s):
        return lax.ppermute(x, "text", [(i, i ^ s) for i in range(texts)])

    packed = (depth // LANES) * rows + 16
    pack = kernel(pack_queries, jax.ShapeDtypeStruct((1, packed, LANES), bf16), 1)
    empty = kernel(blank, jax.ShapeDtypeStruct((TOPK + 1, 8, LANES), f32), 1, flops=4 * 10**9)()
    bundle = pack(query_embed, truth_ids.reshape(1, rows))
    part = own // 2 // PARTS
    sent = kernel(
        pack_texts,
        [jax.ShapeDtypeStruct((part + (8 if n == 0 else 0), depth), bf16) for n in range(PARTS)],
        1,
    )(text_embed, text_ids.reshape(1, own))
    near = [permute(x, PAIR) for x in sent]
    far_bits = []
    s = 2 * PAIR
    while s < texts:
        bundle = jnp.concatenate([bundle, permute(bundle, s)], axis=0)
        far_bits.append(s)
        s *= 2
    tiles = bundle.shape[0]
    bundles = [bundle] + [permute(bundle, d) for d in range(1, PLANE)]

    state_shape = jax.ShapeDtypeStruct((tiles, TOPK + 1, 8, LANES), f32)
    list_shape = jax.ShapeDtypeStruct((16, LANES), f32)
    flops = 2 * own * tiles * LANES * depth
    queries, wanted, state = kernel(
        lambda *refs: rank_own(*refs, tiles=tiles, rows=rows),
        [
            jax.ShapeDtypeStruct((tiles * LANES, depth), bf16),
            jax.ShapeDtypeStruct((tiles, 8, LANES), f32),
            state_shape,
        ],
        12,
        flops=flops,
        scratch_shapes=[pltpu.VMEM((own, tiles * LANES), f32), pltpu.VMEM((own, LANES), f32)],
    )(text_embed, text_ids.reshape(1, own), empty, *bundles)
    far = []
    for x in near:
        far.append(lax.ppermute(x, "query", [(i, i ^ 1) for i in range(cores)]))
    scratch = [pltpu.VMEM((part, tiles * LANES), f32), pltpu.VMEM((part, LANES), f32)]
    flops = flops // 2 // PARTS

    def rank(parts):
        return kernel(
            lambda *refs: rank_parts(*refs, parts=[n for n, m in parts]),
            state_shape,
            8,
            flops=flops * len(parts),
            scratch_shapes=scratch,
        )(
            *[(far if m else near)[n] for n, m in parts],
            *[(far if m else near)[0] for n, m in parts],
            queries,
            wanted,
            state,
        )

    last = PARTS - 1
    if last:
        state = rank([(n, m) for n in range(last) for m in (0, 1)])
    state = rank([(last, 0)])
    lists = kernel(
        lambda *refs: rank_last(*refs, part=last),
        [list_shape] * tiles,
        8,
        flops=flops,
        scratch_shapes=scratch,
    )(far[last], far[0], queries, wanted, state)
    lists = list(lists)
    for s in reversed(far_bits):
        mid = len(lists) // 2
        lists = [
            kernel(join, list_shape, 1)(lists[t], permute(lists[mid + t], s))
            for t in range(mid)
        ]
    mine = lists[0]
    top, margins = kernel(
        lambda *refs: finish(*refs, rows=rows),
        [jax.ShapeDtypeStruct((TOPK, rows), f32), jax.ShapeDtypeStruct((3, rows), f32)],
        1,
    )(mine, *[permute(mine, d) for d in range(1, PLANE)])
    return top.T, margins.T


def solution(mesh):
    texts, cores = mesh.shape["text"], mesh.shape["query"]
    return jax.shard_map(
        lambda *args: per_device(*args, texts=texts, cores=cores),
        mesh=mesh,
        in_specs=(P(("text", "query"), None), P(("text", "query")), P("text", None), P("text")),
        out_specs=(P(("text", "query"), None), P(("text", "query"), None)),
        check_vma=False,
    )
```

```python
import jax
import jax.numpy as jnp
from jax import lax
from jax.experimental import pallas as pl
from jax.experimental.pallas import tpu as pltpu
from jax.sharding import PartitionSpec as P

TOPK = 10
LANES = 128
PLANE = 4
PARTS = 2
PAIR = 4


def exchange(c, i, j):
    c[i], c[j] = jnp.maximum(c[i], c[j]), jnp.minimum(c[i], c[j])


def sort_pairs(n):
    pairs = []
    p = 1
    while p < n:
        k = p
        while k >= 1:
            for j in range(k % p, n - k, 2 * k):
                for i in range(min(k, n - j - k)):
                    if (i + j) // (2 * p) == (i + j + k) // (2 * p):
                        pairs.append((i + j, i + j + k))
            k //= 2
        p *= 2
    return pairs


def sort_top(values):
    c = list(values)
    for i, j in sort_pairs(len(c)):
        exchange(c, i, j)
    return c[:TOPK]


def merge_top(a, b):
    c = [jnp.maximum(a[i], b[TOPK - 1 - i]) for i in range(TOPK)]
    exchange(c, 0, 8)
    exchange(c, 1, 9)
    head = [jnp.maximum(c[0], c[1]), jnp.minimum(c[0], c[1])]
    tail = [c[8], c[9]] + c[2:8]
    for step in (4, 2, 1):
        for i in range(8):
            if i & step == 0:
                exchange(tail, i, i + step)
    return head + tail


def digits_of(ids):
    high = (ids >> 8).astype(jnp.float32)
    low = (ids & 255).astype(jnp.float32)
    row = lax.broadcasted_iota(jnp.int32, (16, ids.shape[1]), 0)
    return jnp.where(row == 0, high, jnp.where(row == 1, low, 0.0)).astype(jnp.bfloat16)


def prepare(query_hbm, wanted_hbm, ids_hbm, block_ref, digits_ref, state_ref, *refs):
    query_ref, wanted_ref, ids_ref, sems = refs
    rows, depth = query_ref.shape
    columns = depth // LANES
    pairs = [(query_hbm, query_ref), (wanted_hbm, wanted_ref), (ids_hbm, ids_ref)]
    copies = [pltpu.make_async_copy(a, b, sems.at[i]) for i, (a, b) in enumerate(pairs)]
    for copy in copies:
        copy.start()
    for i in range(TOPK + 1):
        state_ref[i] = jnp.full((8, LANES), -jnp.inf if i < TOPK else 0.0, jnp.float32)
    for copy in copies:
        copy.wait()
    for j in range(columns):
        block_ref[0, j * rows : (j + 1) * rows, :] = query_ref[:, j * LANES : (j + 1) * LANES]
    ids = jnp.concatenate([wanted_ref[...], jnp.zeros((1, LANES - rows), jnp.int32)], axis=1)
    block_ref[0, columns * rows :, :] = digits_of(ids)
    digits_ref[...] = digits_of(ids_ref[...])


def pack_texts(text_ref, digits_ref, *part_refs):
    part, depth = part_refs[-1].shape
    columns = depth // LANES
    half = part * PARTS
    start = pl.multiple_of(lax.rem(lax.axis_index("query"), 2) * half, half)
    for j in range(columns):
        lanes = slice(j * LANES, (j + 1) * LANES)
        part_refs[0][j * part : (j + 1) * part, :] = text_ref[pl.ds(start, part), lanes]
    spot = columns * part
    digits = digits_ref[:8, pl.ds(start, half)]
    for n in range(half // LANES):
        lanes = slice(n * LANES, (n + 1) * LANES)
        part_refs[0][spot + 8 * n : spot + 8 * n + 8, :] = digits[:, lanes]
    for n in range(1, PARTS):
        part_refs[n][...] = text_ref[pl.ds(pl.multiple_of(start + n * part, part), part), :]


def scan(text_ref, queries, label_ref, score_ref, wanted, states):
    count = score_ref.shape[0]
    piece = min(count, 2 * LANES)
    for r in range(0, count, piece):
        score_ref[r : r + piece, :] = lax.dot_general(
            text_ref[r : r + piece, :],
            queries,
            (((1,), (1,)), ((), ())),
            preferred_element_type=jnp.float32,
        )
    results = []
    for h, state in enumerate(states):
        lanes = slice(h * LANES, (h + 1) * LANES)

        def step(g, carry):
            best, truth = list(carry[:TOPK]), carry[TOPK]
            values = []
            for i in range(16):
                at = pl.ds(pl.multiple_of(g * LANES + i * 8, 8), 8)
                s = score_ref[at, lanes]
                truth = truth + jnp.where(label_ref[at, :] == wanted[h], s, 0.0)
                values.append(s)
            return tuple(merge_top(best, sort_top(values))) + (truth,)

        results.append(lax.fori_loop(0, count // LANES, step, tuple(state)))
    return results


def spread(row, label_ref):
    for i in range(0, row.shape[1], LANES):
        label_ref[i : i + LANES, :] = jnp.broadcast_to(row[:, i : i + LANES], (LANES, LANES)).T


def joined(digits):
    digits = digits.astype(jnp.float32)
    return digits[0:1] * 256.0 + digits[1:2]


def rank_own(*refs, tiles, rows):
    text_ref, ids_ref, blank_ref = refs[:3]
    refs = refs[1:]
    blocks, rests = refs[2 : 2 + PLANE], refs[2 + PLANE : 2 + 2 * PLANE]
    query_ref, wanted_ref, state_ref, score_ref, label_ref = refs[2 + 2 * PLANE :]
    columns = text_ref.shape[1] // LANES
    spread(ids_ref[...].astype(jnp.float32), label_ref)
    wanted = []
    for h in range(tiles):
        total = jnp.zeros((1, LANES), jnp.float32)
        for d in range(PLANE):
            at = slice(h * LANES + d * rows, h * LANES + (d + 1) * rows)
            source = blocks[d].at[0] if h == 0 else rests[d].at[h - 1]
            for j in range(columns):
                query_ref[at, j * LANES : (j + 1) * LANES] = source[j * rows : (j + 1) * rows, :]
            here = joined(source[columns * rows :, :])
            total = total + (here if d == 0 else pltpu.roll(here, d * rows, 1))
        wanted.append(jnp.broadcast_to(total, (8, LANES)))
        wanted_ref[h] = wanted[h]
    start = [blank_ref[i] for i in range(TOPK + 1)]
    states = scan(text_ref, query_ref[...], label_ref, score_ref, wanted, [start] * tiles)
    for h in range(tiles):
        for i in range(TOPK + 1):
            state_ref[h, i] = states[h][i]


def load_states(wanted_ref, state_ref):
    tiles = state_ref.shape[0]
    wanted = [wanted_ref[h] for h in range(tiles)]
    return wanted, [[state_ref[h, i] for i in range(TOPK + 1)] for h in range(tiles)]


def scan_part(part_ref, first_ref, text_ref, query_ref, wanted, states, score_ref, label_ref, part):
    count, depth = text_ref.shape
    columns = depth // LANES
    for n in range(count // LANES):
        at = columns * count + 8 * (part * (count // LANES) + n)
        spread(joined(first_ref[at : at + 8, :]), label_ref.at[pl.ds(n * LANES, LANES)])
    if part == 0:
        for j in range(columns):
            lanes = slice(j * LANES, (j + 1) * LANES)
            text_ref[:, lanes] = part_ref[j * count : (j + 1) * count, :]
        part_ref = text_ref
    return scan(part_ref, query_ref[...], label_ref, score_ref, wanted, states)


def rank_parts(*refs, parts):
    part_refs, refs = refs[: len(parts)], refs[len(parts) :]
    first_refs, refs = refs[: len(parts)], refs[len(parts) :]
    query_ref, wanted_ref, state_ref, next_ref, score_ref, label_ref, text_ref = refs
    wanted, states = load_states(wanted_ref, state_ref)
    for part_ref, first_ref, part in zip(part_refs, first_refs, parts):
        states = scan_part(
            part_ref, first_ref, text_ref, query_ref, wanted, states, score_ref, label_ref, part
        )
    for h, state in enumerate(states):
        for i in range(TOPK + 1):
            next_ref[h, i] = state[i]


def rank_last(part_ref, first_ref, query_ref, wanted_ref, state_ref, *refs, part):
    outs, (score_ref, label_ref, text_ref) = refs[:-3], refs[-3:]
    wanted, states = load_states(wanted_ref, state_ref)
    states = scan_part(
        part_ref, first_ref, text_ref, query_ref, wanted, states, score_ref, label_ref, part
    )
    for out_ref, state in zip(outs, states):
        best, truth = list(state[:TOPK]), state[TOPK]
        for shift in (4, 2, 1):
            best = merge_top(best, [pltpu.roll(b, shift, 0) for b in best])
        for i in range(TOPK):
            out_ref[i : i + 1, :] = best[i][0:1, :]
        out_ref[TOPK : TOPK + 1, :] = jnp.sum(truth, axis=0, keepdims=True)
        out_ref[TOPK + 1 :, :] = jnp.zeros((16 - TOPK - 1, LANES), jnp.float32)


def join(ours_ref, theirs_ref, out_ref):
    best = merge_top(
        [ours_ref[i : i + 1, :] for i in range(TOPK)], [theirs_ref[i : i + 1, :] for i in range(TOPK)]
    )
    for i in range(TOPK):
        out_ref[i : i + 1, :] = best[i]
    out_ref[TOPK : TOPK + 1, :] = ours_ref[TOPK : TOPK + 1, :] + theirs_ref[TOPK : TOPK + 1, :]
    out_ref[TOPK + 1 :, :] = jnp.zeros_like(out_ref[TOPK + 1 :, :])


def finish(*refs, rows):
    lists = []
    for d in range(PLANE):
        x = refs[d][...]
        lists.append(x if d == 0 else pltpu.roll(x, LANES - d * rows, 1))
    top_ref, margin_ref = refs[PLANE:]
    ranks = [[x[i : i + 1, :] for i in range(TOPK)] for x in lists]
    best = merge_top(merge_top(ranks[0], ranks[1]), merge_top(ranks[2], ranks[3]))
    truth = lists[0] + lists[1] + lists[2] + lists[3]
    truth = truth[TOPK : TOPK + 1, :]
    for i in range(TOPK):
        top_ref[i : i + 1, :] = best[i][:, :rows]
    for i, k in enumerate((0, 4, 9)):
        margin_ref[i : i + 1, :] = (truth - best[k])[:, :rows]


def kernel(body, out_shape, mib, flops=0, **extra):
    size = sum(x.size * x.dtype.itemsize for x in jax.tree.leaves(out_shape))
    return pl.pallas_call(
        body,
        out_shape=out_shape,
        compiler_params=pltpu.CompilerParams(vmem_limit_bytes=mib << 20),
        cost_estimate=pl.CostEstimate(flops=flops, bytes_accessed=size, transcendentals=0),
        **extra,
    )


def per_device(query_embed, truth_ids, text_embed, text_ids, texts, cores):
    rows, depth = query_embed.shape
    own = text_embed.shape[0]
    f32, bf16 = jnp.float32, jnp.bfloat16

    def permute(x, s):
        return lax.ppermute(x, "text", [(i, i ^ s) for i in range(texts)])

    packed = (depth // LANES) * rows + 16
    part = own // 2 // PARTS
    inputs = (query_embed, truth_ids.reshape(1, rows), text_ids.reshape(1, own))
    block, digits, empty = kernel(
        prepare,
        [
            jax.ShapeDtypeStruct((1, packed, LANES), bf16),
            jax.ShapeDtypeStruct((16, own), bf16),
            jax.ShapeDtypeStruct((TOPK + 1, 8, LANES), f32),
        ],
        1,
        flops=4 * 10**9,
        in_specs=[pl.BlockSpec(memory_space=pltpu.HBM)] * 3,
        scratch_shapes=[
            pltpu.VMEM((rows, depth), bf16),
            pltpu.VMEM((1, rows), jnp.int32),
            pltpu.VMEM((1, own), jnp.int32),
            pltpu.SemaphoreType.DMA((3,)),
        ],
    )(*[pltpu.with_memory_space_constraint(x, pltpu.HBM) for x in inputs])
    first_rows = (depth // LANES) * part + 8 * (own // 2 // LANES)
    sent = kernel(
        pack_texts,
        [jax.ShapeDtypeStruct((first_rows, LANES), bf16)]
        + [jax.ShapeDtypeStruct((part, depth), bf16)] * (PARTS - 1),
        1,
    )(text_embed, digits)
    near = [permute(x, PAIR) for x in sent]
    blocks = [block] + [permute(block, d) for d in range(1, PLANE)]
    far_bits = [2 * PAIR]
    rest = permute(block, 2 * PAIR)
    s = 4 * PAIR
    while s < texts:
        new, more = permute(block, s), permute(rest, s)
        rest = jnp.concatenate([rest, new, more], axis=0)
        far_bits.append(s)
        s *= 2
    tiles = 1 + rest.shape[0]
    rests = [rest] + [permute(rest, d) for d in range(1, PLANE)]

    state_shape = jax.ShapeDtypeStruct((tiles, TOPK + 1, 8, LANES), f32)
    list_shape = jax.ShapeDtypeStruct((16, LANES), f32)
    flops = 2 * own * tiles * LANES * depth
    queries, wanted, state = kernel(
        lambda *refs: rank_own(*refs, tiles=tiles, rows=rows),
        [
            jax.ShapeDtypeStruct((tiles * LANES, depth), bf16),
            jax.ShapeDtypeStruct((tiles, 8, LANES), f32),
            state_shape,
        ],
        12,
        flops=flops,
        scratch_shapes=[pltpu.VMEM((own, tiles * LANES), f32), pltpu.VMEM((own, LANES), f32)],
    )(text_embed, text_ids.reshape(1, own), empty, *blocks, *rests)
    far = []
    for x in near:
        far.append(lax.ppermute(x, "query", [(i, i ^ 1) for i in range(cores)]))
    scratch = [
        pltpu.VMEM((part, tiles * LANES), f32),
        pltpu.VMEM((part, LANES), f32),
        pltpu.VMEM((part, depth), bf16),
    ]
    flops = flops // 2 // PARTS

    def rank(parts):
        return kernel(
            lambda *refs: rank_parts(*refs, parts=[n for n, m in parts]),
            state_shape,
            8,
            flops=flops * len(parts),
            scratch_shapes=scratch,
        )(
            *[(far if m else near)[n] for n, m in parts],
            *[(far if m else near)[0] for n, m in parts],
            queries,
            wanted,
            state,
        )

    last = PARTS - 1
    if last:
        state = rank([(n, m) for n in range(last) for m in (0, 1)])
    state = rank([(last, 0)])
    lists = kernel(
        lambda *refs: rank_last(*refs, part=last),
        [list_shape] * tiles,
        8,
        flops=flops,
        scratch_shapes=scratch,
    )(far[last], far[0], queries, wanted, state)
    lists = list(lists)
    for s in reversed(far_bits):
        mid = len(lists) // 2
        lists = [
            kernel(join, list_shape, 1)(lists[t], permute(lists[mid + t], s))
            for t in range(mid)
        ]
    mine = lists[0]
    top, margins = kernel(
        lambda *refs: finish(*refs, rows=rows),
        [jax.ShapeDtypeStruct((TOPK, rows), f32), jax.ShapeDtypeStruct((3, rows), f32)],
        1,
    )(mine, *[permute(mine, d) for d in range(1, PLANE)])
    return top.T, margins.T


def solution(mesh):
    texts, cores = mesh.shape["text"], mesh.shape["query"]
    return jax.shard_map(
        lambda *args: per_device(*args, texts=texts, cores=cores),
        mesh=mesh,
        in_specs=(P(("text", "query"), None), P(("text", "query")), P("text", None), P("text")),
        out_specs=(P(("text", "query"), None), P(("text", "query"), None)),
        check_vma=False,
    )
```
